16 devices in a mesh: dp: 2 (over y, z), sp: 8 (over x, core).
Axes of the slice: x: 4, y: 2, z: 1, core: 2. Of those that a mesh axis runs over, the one named last changes fastest.
The devices are a block of a 4x4x8 slice.
Arguments:
- x: bfloat16 [8192, 3072], P(('dp', 'sp')), parts along dimension 0
- grad_out: bfloat16 [8192, 3072], P(('dp', 'sp')), parts along dimension 0
- positions: int32 [8192], P(('dp', 'sp')), parts along dimension 0
- gain: bfloat16 [3072], replicated
- w_q: bfloat16 [3072, 3072], replicated
- w_k: bfloat16 [3072, 1024], replicated
- w_v: bfloat16 [3072, 1024], replicated
- w_o: bfloat16 [3072, 3072], replicated
Outputs:
- output 1: bfloat16 [8192, 3072], P(('dp', 'sp')), parts along dimension 0
- output 2: bfloat16 [8192, 3072], P(('dp', 'sp')), parts along dimension 0
- output 3: float32 [6144, 3072], P('dp'), parts along dimension 0
- output 4: float32 [6144, 1024], P('dp'), parts along dimension 0
- output 5: float32 [6144, 1024], P('dp'), parts along dimension 0
- output 6: float32 [6144, 3072], P('dp'), parts along dimension 0
- output 7: float32 [6144], P('dp'), parts along dimension 0
There are 2 independent parts. The reference program is written for one: setup_inputs(seed, part) draws one part's arguments, and reference() takes and returns one part's arrays. A program takes and returns all parts, laid end to end along the dimension named above; an argument that names none is the same for every part.
All inputs are finite; a program needn't handle non-finite values.
Results may differ from the reference program's by a relative error of at most 0.0183642.
Values are sent between devices in bfloat16 or wider.
A program may use at most 768 MiB of HBM per device.

```python
import jax
import jax.numpy as jnp
from jax import lax

D = 3072
HEADS = 24
KV_HEADS = 8
HEAD = 128
SEQ = 4096
GROUP = HEADS // KV_HEADS
ROPE_THETA = 1000000.0
NORM_EPS = 1e-05
NEG_LARGE = -1e30


def block_rows(seq_len, row_cost):
    row_count = seq_len
    while row_count > 8 and row_count * row_cost > 2 ** 24:
        row_count = row_count // 2
    return row_count


def setup_inputs(seed: int = 0, part: int = 0) -> dict:
    base_key = jax.random.key(seed)
    part_key = jax.random.fold_in(base_key, part)
    key_x, key_dy, key_start, key_step = jax.random.split(part_key, 4)
    shared = jax.random.split(jax.random.key(seed + 1), 5)
    x = jax.random.normal(key_x, (SEQ, D), jnp.float32).astype(jnp.bfloat16)
    grad_out = jax.random.normal(key_dy, (SEQ, D), jnp.float32).astype(jnp.bfloat16)
    pos_start = jax.random.randint(key_start, (), 0, SEQ)
    pos_steps = jax.random.randint(key_step, (SEQ,), 1, 4)
    positions = (pos_start + jnp.cumsum(pos_steps) - pos_steps[0]).astype(jnp.int32)
    gain = (1.0 + 0.3 * jax.random.normal(shared[0], (D,), jnp.float32)).astype(jnp.bfloat16)
    w_q = (jax.random.normal(shared[1], (D, HEADS * HEAD), jnp.float32) * D ** -0.5).astype(jnp.bfloat16)
    w_k = (jax.random.normal(shared[2], (D, KV_HEADS * HEAD), jnp.float32) * D ** -0.5).astype(jnp.bfloat16)
    w_v = (jax.random.normal(shared[3], (D, KV_HEADS * HEAD), jnp.float32) * D ** -0.5).astype(jnp.bfloat16)
    w_o = (jax.random.normal(shared[4], (HEADS * HEAD, D), jnp.float32) * (HEADS * HEAD) ** -0.5).astype(jnp.bfloat16)
    return {'x': x, 'grad_out': grad_out, 'positions': positions, 'gain': gain, 'w_q': w_q, 'w_k': w_k, 'w_v': w_v, 'w_o': w_o}


def rope(values, cos_t, sin_t):
    half_dim = HEAD // 2
    lower_half = values[..., :half_dim]
    upper_half = values[..., half_dim:]
    return jnp.concatenate([lower_half * cos_t - upper_half * sin_t, upper_half * cos_t + lower_half * sin_t], axis=-1)


def attend(q_all, k_all, v_all):
    row_count = block_rows(SEQ, HEADS * SEQ)
    n_blocks = SEQ // row_count
    key_f = k_all.astype(jnp.float32)
    val_f = v_all.astype(jnp.float32)
    key_index = jnp.arange(SEQ)
    q_blocks = q_all.reshape(n_blocks, row_count, KV_HEADS, GROUP, HEAD)
    blk_starts = jnp.arange(n_blocks) * row_count

    def one_block(block_args):
        q_blk, blk_start = block_args
        scores = jnp.einsum('qhgd,khd->hgqk', q_blk.astype(jnp.float32), key_f) * HEAD ** -0.5
        causal = (blk_start + jnp.arange(row_count))[:, None] >= key_index[None, :]
        attn_prob = jax.nn.softmax(jnp.where(causal, scores, NEG_LARGE), axis=-1)
        blk_out = jnp.einsum('hgqk,khd->qhgd', attn_prob.astype(jnp.bfloat16).astype(jnp.float32), val_f)
        return blk_out.astype(jnp.bfloat16)

    outputs = lax.map(jax.checkpoint(one_block), (q_blocks, blk_starts))
    return outputs.reshape(SEQ, KV_HEADS, GROUP, HEAD)


def reference(x, grad_out, positions, gain, w_q, w_k, w_v, w_o):
    inv_freq = ROPE_THETA ** (-jnp.arange(0, HEAD, 2).astype(jnp.float32) / HEAD)
    angles = positions.astype(jnp.float32)[:, None] * inv_freq[None, :]
    cos_t = jnp.cos(angles)[:, None, :]
    sin_t = jnp.sin(angles)[:, None, :]

    def forward(x_f, gain_f, wq_f, wk_f, wv_f, wo_f):
        normed = x_f * lax.rsqrt(jnp.mean(x_f * x_f, axis=-1, keepdims=True) + NORM_EPS)
        hidden = (normed * gain_f).astype(jnp.bfloat16).astype(jnp.float32)
        q_proj = jnp.dot(hidden, wq_f, preferred_element_type=jnp.float32).reshape(SEQ, HEADS, HEAD)
        k_proj = jnp.dot(hidden, wk_f, preferred_element_type=jnp.float32).reshape(SEQ, KV_HEADS, HEAD)
        v_all = jnp.dot(hidden, wv_f, preferred_element_type=jnp.float32).astype(jnp.bfloat16).reshape(SEQ, KV_HEADS, HEAD)
        q_all = rope(q_proj, cos_t, sin_t).astype(jnp.bfloat16).reshape(SEQ, KV_HEADS, GROUP, HEAD)
        k_all = rope(k_proj, cos_t, sin_t).astype(jnp.bfloat16)
        attn = attend(q_all, k_all, v_all).reshape(SEQ, HEADS * HEAD)
        mixed = jnp.dot(attn.astype(jnp.float32), wo_f, preferred_element_type=jnp.float32)
        return (x_f + mixed).astype(jnp.bfloat16)

    result, pullback = jax.vjp(forward, x.astype(jnp.float32), gain.astype(jnp.float32), w_q.astype(jnp.float32), w_k.astype(jnp.float32), w_v.astype(jnp.float32), w_o.astype(jnp.float32))
    grad_xf, grad_gain, grad_wq, grad_wk, grad_wv, grad_wo = pullback(grad_out)
    return result, grad_xf.astype(jnp.bfloat16), grad_wq, grad_wk, grad_wv, grad_wo, grad_gain
```

```python
import functools

import jax
import jax.numpy as jnp
from jax import lax
from jax.experimental import pallas as pl
from jax.experimental.pallas import tpu as pltpu
from jax.sharding import PartitionSpec as P

HEAD = 128
HALF = HEAD // 2
ROPE_THETA = 1000000.0
NORM_EPS = 1e-05
NEG_LARGE = -1e30
LOG2E = 1.4426950408889634
QK_SCALE = HEAD ** -0.5
EXP_SCALE = QK_SCALE * LOG2E
BLK = 512
F32 = jnp.float32
BF16 = jnp.bfloat16
VMEM_MAX = 60 * 2 ** 20
NN = (((1,), (0,)), ((), ()))
NT = (((1,), (1,)), ((), ()))
TN = (((0,), (0,)), ((), ()))


def dot(a, b, dims=NN):
    return lax.dot_general(a, b, dims, preferred_element_type=F32)


def params(limit=VMEM_MAX):
    return pltpu.CompilerParams(vmem_limit_bytes=limit)


def cost(flops, nbytes):
    return pl.CostEstimate(flops=int(flops), bytes_accessed=int(nbytes), transcendentals=0)


def qkv_kernel(q_heads, wT_ref, hT_ref, cos_ref, sin_ref, q_ref, qT_ref, k_ref, kT_ref, vT_ref):
    projT = dot(wT_ref[...], hT_ref[0])
    cos_t = cos_ref[...]
    sin_t = sin_ref[...]

    def rope(block):
        low, high = block[:HALF], block[HALF:]
        return jnp.concatenate([low * cos_t - high * sin_t, high * cos_t + low * sin_t], axis=0)

    for head in range(q_heads):
        rot = rope(projT[head * HEAD:(head + 1) * HEAD])
        qT_ref[head] = rot.astype(BF16)
        q_ref[head] = rot.T.astype(BF16)
    base = q_heads * HEAD
    rot = rope(projT[base:base + HEAD])
    kT_ref[...] = rot.astype(BF16)
    k_ref[...] = rot.T.astype(BF16)
    vT_ref[...] = projT[base + HEAD:base + 2 * HEAD].astype(BF16)


def qkv_call(wT, hT_all, cosT, sinT, q_heads):
    shards, d_model, tok = hT_all.shape
    seq = shards * tok
    rows = wT.shape[0]
    return pl.pallas_call(
        functools.partial(qkv_kernel, q_heads),
        grid=(shards,),
        in_specs=[pl.BlockSpec((rows, d_model), lambda j: (0, 0)),
                  pl.BlockSpec((1, d_model, tok), lambda j: (j, 0, 0)),
                  pl.BlockSpec((HALF, tok), lambda j: (0, j)),
                  pl.BlockSpec((HALF, tok), lambda j: (0, j))],
        out_specs=[pl.BlockSpec((q_heads, tok, HEAD), lambda j: (0, j, 0)),
                   pl.BlockSpec((q_heads, HEAD, tok), lambda j: (0, 0, j)),
                   pl.BlockSpec((tok, HEAD), lambda j: (j, 0)),
                   pl.BlockSpec((HEAD, tok), lambda j: (0, j)),
                   pl.BlockSpec((HEAD, tok), lambda j: (0, j))],
        out_shape=[jax.ShapeDtypeStruct((q_heads, seq, HEAD), BF16),
                   jax.ShapeDtypeStruct((q_heads, HEAD, seq), BF16),
                   jax.ShapeDtypeStruct((seq, HEAD), BF16),
                   jax.ShapeDtypeStruct((HEAD, seq), BF16),
                   jax.ShapeDtypeStruct((HEAD, seq), BF16)],
        compiler_params=params(),
        cost_estimate=cost(2 * rows * d_model * seq, 2 * d_model * seq),
        name='qkv',
    )(wT, hT_all, cosT, sinT)


def fwd_kernel(q_heads, qT_ref, k_ref, vT_ref, oT_ref, lse_ref, m_ref, l_ref, acc_ref):
    i = pl.program_id(0)
    m_ref[...] = jnp.full(m_ref.shape, NEG_LARGE, F32)
    l_ref[...] = jnp.zeros(l_ref.shape, F32)
    acc_ref[...] = jnp.zeros(acc_ref.shape, F32)

    def step(j, masked):
        rows = pl.ds(pl.multiple_of(j * BLK, BLK), BLK)
        k_blk = k_ref[rows, :]
        vT_blk = vT_ref[:, rows]
        for head in range(q_heads):
            s = dot(k_blk, qT_ref[head])
            if masked:
                key = lax.broadcasted_iota(jnp.int32, s.shape, 0)
                qry = lax.broadcasted_iota(jnp.int32, s.shape, 1)
                s = jnp.where(key <= qry, s, NEG_LARGE)
            m_old = m_ref[head]
            m_new = jnp.maximum(m_old, jnp.max(s, axis=0, keepdims=True))
            m_ref[head] = m_new
            p = jnp.exp2(s * EXP_SCALE - m_new * EXP_SCALE)
            alpha = jnp.exp2((m_old - m_new) * EXP_SCALE)
            l_ref[head] = l_ref[head] * alpha + jnp.sum(p, axis=0, keepdims=True)
            acc_ref[head] = acc_ref[head] * alpha + dot(vT_blk, p.astype(BF16))

    lax.fori_loop(0, i, lambda j, _: (step(j, False), 0)[1], 0)
    step(i, True)
    for head in range(q_heads):
        l = l_ref[head]
        oT_ref[head] = (acc_ref[head] / l).astype(BF16)
        lse = m_ref[head] * EXP_SCALE + jnp.log2(l)
        lse_ref[head] = jnp.broadcast_to(lse, (HEAD, BLK)).T


def fwd_call(qT, k, vT):
    q_heads, _, seq = qT.shape
    n_blk = seq // BLK
    return pl.pallas_call(
        functools.partial(fwd_kernel, q_heads),
        grid=(n_blk,),
        in_specs=[pl.BlockSpec((q_heads, HEAD, BLK), lambda i: (0, 0, i)),
                  pl.BlockSpec((seq, HEAD), lambda i: (0, 0)),
                  pl.BlockSpec((HEAD, seq), lambda i: (0, 0))],
        out_specs=[pl.BlockSpec((q_heads, HEAD, BLK), lambda i: (0, 0, i)),
                   pl.BlockSpec((q_heads, BLK, HEAD), lambda i: (0, i, 0))],
        out_shape=[jax.ShapeDtypeStruct((q_heads, HEAD, seq), BF16),
                   jax.ShapeDtypeStruct((q_heads, seq, HEAD), F32)],
        scratch_shapes=[pltpu.VMEM((q_heads, 1, BLK), F32),
                        pltpu.VMEM((q_heads, 1, BLK), F32),
                        pltpu.VMEM((q_heads, HEAD, BLK), F32)],
        compiler_params=params(),
        cost_estimate=cost(4 * q_heads * HEAD * seq * seq, 4 * q_heads * HEAD * seq),
        name='attn_fwd',
    )(qT, k, vT)


def do_kernel(q_heads, dy_ref, woT_ref, oT_ref, do_ref, doT_ref, delta_ref):
    d_o = dot(dy_ref[...], woT_ref[...])
    for head in range(q_heads):
        blk = d_o[:, head * HEAD:(head + 1) * HEAD].astype(BF16)
        blkT = blk.astype(F32).T
        do_ref[head] = blk
        doT_ref[head] = blkT.astype(BF16)
        delta = jnp.sum(blkT * oT_ref[head].astype(F32), axis=0, keepdims=True)
        delta_ref[head] = jnp.broadcast_to(delta, (HEAD, delta.shape[1])).T


def do_call(dy_all, woT, oT):
    seq, d_model = dy_all.shape
    q_heads = oT.shape[0]
    return pl.pallas_call(
        functools.partial(do_kernel, q_heads),
        grid=(seq // BLK,),
        in_specs=[pl.BlockSpec((BLK, d_model), lambda i: (i, 0)),
                  pl.BlockSpec((d_model, q_heads * HEAD), lambda i: (0, 0)),
                  pl.BlockSpec((q_heads, HEAD, BLK), lambda i: (0, 0, i))],
        out_specs=[pl.BlockSpec((q_heads, BLK, HEAD), lambda i: (0, i, 0)),
                   pl.BlockSpec((q_heads, HEAD, BLK), lambda i: (0, 0, i)),
                   pl.BlockSpec((q_heads, BLK, HEAD), lambda i: (0, i, 0))],
        out_shape=[jax.ShapeDtypeStruct((q_heads, seq, HEAD), BF16),
                   jax.ShapeDtypeStruct((q_heads, HEAD, seq), BF16),
                   jax.ShapeDtypeStruct((q_heads, seq, HEAD), F32)],
        compiler_params=params(),
        cost_estimate=cost(2 * seq * d_model * q_heads * HEAD, 2 * seq * d_model),
        name='d_o',
    )(dy_all, woT, oT)


def bwd_kernel(first, last, n_blk, *refs):
    (q_ref, qT_ref, do_ref, doT_ref, lse_ref, delta_ref, k_ref, kT_ref, vT_ref,
     cos_ref, sin_ref, cosT_ref, sinT_ref) = refs[:13]
    refs = refs[13:]
    if not first:
        dk_in, dv_in = refs[:2]
        refs = refs[2:]
    dq_ref, dk_out, dv_out, dq_acc, dk_acc, dv_acc = refs
    j = pl.program_id(0)

    @pl.when(j == 0)
    def _():
        dq_acc[...] = jnp.zeros(dq_acc.shape, F32)

    if first:
        dk_acc[...] = jnp.zeros(dk_acc.shape, F32)
        dv_acc[...] = jnp.zeros(dv_acc.shape, F32)
    else:
        dk_acc[...] = dk_in[...]
        dv_acc[...] = dv_in[...]
    k_blk = k_ref[...]
    kT_blk = kT_ref[...]
    vT_blk = vT_ref[...]

    def step(i, masked):
        rows = pl.ds(pl.multiple_of(i * BLK, BLK), BLK)
        s = dot(q_ref[0, rows, :], kT_blk)
        dp = dot(do_ref[0, rows, :], vT_blk)
        lse = lse_ref[0, rows, :]
        delta = delta_ref[0, rows, :]
        reps = BLK // HEAD
        p = jnp.exp2(s * EXP_SCALE - jnp.concatenate([lse] * reps, axis=1))
        if masked:
            qry = lax.broadcasted_iota(jnp.int32, s.shape, 0)
            key = lax.broadcasted_iota(jnp.int32, s.shape, 1)
            p = jnp.where(key <= qry, p, 0.0)
        ds = p * (dp - jnp.concatenate([delta] * reps, axis=1))
        p_bf = p.astype(BF16)
        ds_bf = ds.astype(BF16)
        dv_acc[...] += dot(doT_ref[0, :, rows], p_bf)
        dk_acc[...] += dot(qT_ref[0, :, rows], ds_bf)
        dq_acc[rows, :] += dot(ds_bf, k_blk)

    step(j, True)
    lax.fori_loop(j + 1, n_blk, lambda i, _: (step(i, False), 0)[1], 0)
    rows = pl.ds(pl.multiple_of(j * BLK, BLK), BLK)
    dq = dq_acc[rows, :] * QK_SCALE
    dq_ref[...] = (dq * cos_ref[...] + pltpu.roll(dq, HALF, 1) * sin_ref[...]).astype(BF16)
    if last:
        dk = dk_acc[...] * QK_SCALE
        low, high = dk[:HALF], dk[HALF:]
        cos_t, sin_t = cosT_ref[...], sinT_ref[...]
        pre = jnp.concatenate([low * cos_t + high * sin_t, high * cos_t - low * sin_t], axis=0)
        dk_out[...] = pre.T.astype(BF16)
        dv_out[...] = dv_acc[...].T.astype(BF16)
    else:
        dk_out[...] = dk_acc[...]
        dv_out[...] = dv_acc[...]


def bwd_call(head, n_heads, ops, dkv):
    q, qT, d_o, doT, lse, delta, k, kT, vT, cos, sin, cosT, sinT = ops
    seq = k.shape[0]
    n_blk = seq // BLK
    first, last = head == 0, head == n_heads - 1
    row_all = pl.BlockSpec((1, seq, HEAD), lambda j: (head, 0, 0))
    colT_all = pl.BlockSpec((1, HEAD, seq), lambda j: (head, 0, 0))
    row_blk = pl.BlockSpec((BLK, HEAD), lambda j: (j, 0))
    colT_blk = pl.BlockSpec((HEAD, BLK), lambda j: (0, j))
    half_blk = pl.BlockSpec((HALF, BLK), lambda j: (0, j))
    in_specs = [row_all, colT_all, row_all, colT_all, row_all, row_all,
                row_blk, colT_blk, colT_blk, row_blk, row_blk, half_blk, half_blk]
    args = list(ops)
    if not first:
        in_specs += [colT_blk, colT_blk]
        args += list(dkv)
    if last:
        kv_spec, kv_shape = row_blk, jax.ShapeDtypeStruct((seq, HEAD), BF16)
    else:
        kv_spec, kv_shape = colT_blk, jax.ShapeDtypeStruct((HEAD, seq), F32)
    dq, dk, dv = pl.pallas_call(
        functools.partial(bwd_kernel, first, last, n_blk),
        grid=(n_blk,),
        in_specs=in_specs,
        out_specs=[row_blk, kv_spec, kv_spec],
        out_shape=[jax.ShapeDtypeStruct((seq, HEAD), BF16), kv_shape, kv_shape],
        scratch_shapes=[pltpu.VMEM((seq, HEAD), F32), pltpu.VMEM((HEAD, BLK), F32), pltpu.VMEM((HEAD, BLK), F32)],
        compiler_params=params(),
        cost_estimate=cost(10 * HEAD * seq * seq, 12 * HEAD * seq),
        name='attn_bwd',
    )(*args)
    return dq, (dk, dv)


def dw_kernel(shards, tok, row_blk, stride, offset, aliased, *refs):
    hT_any, d_any = refs[:2]
    out_any, lhs, rhs, acc, lhs_sem, rhs_sem, out_sem = refs[2 + aliased:]
    d_model = hT_any.shape[1]
    steps = d_model // row_blk

    def lhs_copy(step, slot, j):
        return pltpu.make_async_copy(hT_any.at[j, pl.ds(step * row_blk, row_blk), :],
                                     lhs.at[slot, :, pl.ds(j * tok, tok)], lhs_sem.at[slot, j])

    def rhs_copy(j):
        return pltpu.make_async_copy(d_any.at[j], rhs.at[:, pl.ds(j * HEAD, HEAD)], rhs_sem.at[j])

    def out_copy(step, slot, j):
        return pltpu.make_async_copy(
            acc.at[slot, :, pl.ds(j * HEAD, HEAD)],
            out_any.at[pl.ds(step * row_blk, row_blk), pl.ds((j * stride + offset) * HEAD, HEAD)],
            out_sem.at[slot, j])

    for j in range(shards):
        lhs_copy(0, 0, j).start()
    for j in range(shards):
        rhs_copy(j).start()
    for step in range(steps):
        slot = step % 2
        if step + 1 < steps:
            for j in range(shards):
                lhs_copy(step + 1, 1 - slot, j).start()
        for j in range(shards):
            lhs_copy(step, slot, j).wait()
        if step >= 2:
            for j in range(shards):
                out_copy(step - 2, slot, j).wait()
        for pair in range(shards // 2):
            if step == 0:
                rhs_copy(2 * pair).wait()
                rhs_copy(2 * pair + 1).wait()
            cols = pl.ds(pair * 2 * HEAD, 2 * HEAD)
            acc[slot, :, cols] = dot(lhs[slot], rhs[:, cols])
            out_copy(step, slot, 2 * pair).start()
            out_copy(step, slot, 2 * pair + 1).start()
    for step in range(max(0, steps - 2), steps):
        for j in range(shards):
            out_copy(step, step % 2, j).wait()


def dw_call(hT_all, d_all, stride, offset, width, prev):
    shards, d_model, tok = hT_all.shape
    seq = shards * tok
    row_blk = 512
    aliased = 0 if prev is None else 1
    args = [hT_all, d_all] + ([] if prev is None else [prev])
    return pl.pallas_call(
        functools.partial(dw_kernel, shards, tok, row_blk, stride, offset, aliased),
        in_specs=[pl.BlockSpec(memory_space=pl.ANY)] * len(args),
        out_specs=pl.BlockSpec(memory_space=pl.ANY),
        out_shape=jax.ShapeDtypeStruct((d_model, width), F32),
        scratch_shapes=[pltpu.VMEM((2, row_blk, seq), BF16),
                        pltpu.VMEM((seq, shards * HEAD), BF16),
                        pltpu.VMEM((2, row_blk, shards * HEAD), F32),
                        pltpu.SemaphoreType.DMA((2, shards)),
                        pltpu.SemaphoreType.DMA((shards,)),
                        pltpu.SemaphoreType.DMA((2, shards))],
        input_output_aliases={} if prev is None else {2: 0},
        compiler_params=params(),
        cost_estimate=cost(2 * seq * d_model * shards * HEAD, 2 * seq * (d_model + shards * HEAD)),
        name='d_w',
    )(*args)


def solution(mesh):
    sp_size = mesh.shape['sp']
    seq_spec = P(('dp', 'sp'), None)
    replicated = P(None, None)
    part_rows = P('dp', None)

    def local_step(x, grad_out, positions, gain, w_q, w_k, w_v, w_o):
        tok, d_model = x.shape
        n_heads = w_q.shape[1] // HEAD
        q_loc = n_heads // sp_size
        seq = tok * sp_size
        me = lax.axis_index('sp')
        x_f = x.astype(F32)
        inv_rms = lax.rsqrt(jnp.mean(x_f * x_f, axis=-1, keepdims=True) + NORM_EPS)
        normed = x_f * inv_rms
        gain_f = gain.astype(F32)
        hidden = (normed * gain_f).astype(BF16)
        hT_all = lax.all_gather(hidden.T, 'sp', axis=0)
        pos_all = lax.all_gather(positions, 'sp', axis=0, tiled=True)
        dy_src, _ = lax.optimization_barrier((grad_out, hidden))
        dy_all = lax.all_gather(dy_src, 'sp', axis=0, tiled=True)

        inv_freq = ROPE_THETA ** (-jnp.arange(0, HEAD, 2).astype(F32) / HEAD)
        anglesT = inv_freq[:, None] * pos_all.astype(F32)[None, :]
        cosT, sinT = jnp.cos(anglesT), jnp.sin(anglesT)
        cos = jnp.concatenate([cosT, cosT], axis=0).T
        sin = jnp.concatenate([sinT, -sinT], axis=0).T

        q_cols = q_loc * HEAD
        wq_own = lax.dynamic_slice_in_dim(w_q, me * q_cols, q_cols, 1)
        wk_own = lax.dynamic_slice_in_dim(w_k, me * HEAD, HEAD, 1)
        wv_own = lax.dynamic_slice_in_dim(w_v, me * HEAD, HEAD, 1)
        wT = jnp.concatenate([wq_own, wk_own, wv_own], axis=1).T
        woT = lax.dynamic_slice_in_dim(w_o, me * q_cols, q_cols, 0).T

        q, qT, k, kT, vT = qkv_call(wT, hT_all, cosT, sinT, q_loc)
        oT, lse = fwd_call(qT, k, vT)
        oT_all = lax.all_gather(oT, 'sp', axis=0).reshape(n_heads * HEAD, seq)
        d_o, doT, delta = do_call(dy_all, woT, oT)
        ops = (q, qT, d_o, doT, lse, delta, k, kT, vT, cos, sin, cosT, sinT)
        dkv = None
        dq_alls = []
        for head in range(q_loc):
            dq, dkv = bwd_call(head, q_loc, ops, dkv)
            dq_alls.append(lax.all_gather(dq, 'sp', axis=0))
        dk_all = lax.all_gather(dkv[0], 'sp', axis=0)
        dv_all = lax.all_gather(dkv[1], 'sp', axis=0)

        oT_loc = lax.dynamic_slice_in_dim(oT_all, me * tok, tok, 1)
        mixed = dot(oT_loc, w_o, TN)
        result = (x_f + mixed).astype(BF16)
        grad_wo = dot(oT_all, dy_all)

        grad_wq = None
        for head in range(q_loc):
            grad_wq = dw_call(hT_all, dq_alls[head], q_loc, head, n_heads * HEAD, grad_wq)
        grad_wk = dw_call(hT_all, dk_all, 1, 0, sp_size * HEAD, None)
        grad_wv = dw_call(hT_all, dv_all, 1, 0, sp_size * HEAD, None)

        def own(d_all):
            return lax.dynamic_slice_in_dim(d_all, me * tok, tok, 1)

        dq_own = jnp.stack([own(d) for d in dq_alls], axis=1)
        dq_own = dq_own.transpose(2, 0, 1, 3).reshape(tok, n_heads * HEAD)
        dk_own = own(dk_all).transpose(1, 0, 2).reshape(tok, sp_size * HEAD)
        dv_own = own(dv_all).transpose(1, 0, 2).reshape(tok, sp_size * HEAD)
        d_hidden = dot(dq_own, w_q, NT) + dot(dk_own, w_k, NT) + dot(dv_own, w_v, NT)
        grad_gain = lax.psum(jnp.sum(d_hidden * normed, axis=0), 'sp')
        d_normed = d_hidden * gain_f
        d_xnorm = inv_rms * (d_normed - normed * jnp.mean(d_normed * normed, axis=-1, keepdims=True))
        grad_x = (grad_out.astype(F32) + d_xnorm).astype(BF16)
        return result, grad_x, grad_wq, grad_wk, grad_wv, grad_wo, grad_gain

    return jax.shard_map(local_step, mesh=mesh,
                         in_specs=(seq_spec, seq_spec, P(('dp', 'sp')), P(None),
                                   replicated, replicated, replicated, replicated),
                         out_specs=(seq_spec, seq_spec, part_rows, part_rows, part_rows, part_rows, P('dp')),
                         check_vma=False)
```
